32 devices in a mesh: dp: 8 (over y, x, core), tensor: 4 (over z).
Axes of the slice: x: 2, y: 2, z: 4, core: 2. Of those that a mesh axis runs over, the one named last changes fastest.
Arguments:
- img_hidden: bfloat16 [4096, 4304], P('dp', 'tensor'), may hold values from -0.25 to 0.25
- img_down: bfloat16 [4304, 1152], P('tensor'), may hold values from -0.09375 to 0.09375
- img_pooled: bfloat16 [4096, 1152], P(('dp', 'tensor')), may hold values from -0.25 to 0.25
- txt_hidden: bfloat16 [4096, 1152], P('dp', 'tensor'), may hold values from -0.25 to 0.25
- txt_proj: bfloat16 [1152, 1152], P('tensor'), may hold values from -0.1875 to 0.1875
- log_temp: float32 [1], replicated, may hold values from 1 to 2
- bias: float32 [1], replicated, may hold values from -4 to -1
- match: int32 [4096], P(('dp', 'tensor')), may hold values from 0 to 4095
- window_index: int32 [1], replicated, may hold values from 0 to 1
Outputs:
- img_grad: float32 [4096, 1152], P(('dp', 'tensor'))
- txt_grad: float32 [4096, 1152], P(('dp', 'tensor'))
- row_loss: float32 [4096], P(('dp', 'tensor'))
The draws below stay inside these ranges and needn't reach their ends.
All inputs are finite; a program needn't handle non-finite values.
Results may differ from the reference program's by a relative error of at most 0.0039.
Values may be sent and summed in bfloat16 or wider, within the bound.
A program may use at most 64 MiB of HBM per device.

```python
import jax
import jax.numpy as jnp
from jax import lax

D = 1152
K_IMG = 4304
K_TXT = 1152
ROWS = 128
STEPS = 16
BATCH = 4096
WINDOWS = 2
N_DP = 8
N_TENSOR = 4


def plant(values, key, low, top_value):
    spot = [jax.random.randint(jax.random.fold_in(key, axis), (), 0, length) for axis, length in enumerate(values.shape)]
    main_axis = values.shape.index(max(values.shape))
    neighbour = spot[:main_axis] + [(spot[main_axis] + 1) % values.shape[main_axis]] + spot[main_axis + 1:]
    return values.at[tuple(spot)].set(low).at[tuple(neighbour)].set(top_value)


def block_scale(stream_key, dims, shards, smallest, largest):
    level = 1.0
    for dim, parts in shards:
        steps = jax.random.uniform(jax.random.fold_in(jax.random.fold_in(stream_key, 6), dim), (parts,), jnp.float32, smallest / len(shards), largest / len(shards))
        level = level * jnp.repeat(jnp.exp(steps), dims[dim] // parts).reshape((-1,) + (1,) * (len(dims) - 1 - dim))
    return level


def noise(rng, shape, scale, bound, split=(), kind=jnp.bfloat16):
    gain = block_scale(rng, shape, split, -0.22, 0.18) if split else 1.0
    array = jax.random.normal(rng, shape, jnp.float32) * scale * gain
    return jnp.minimum(jnp.maximum(array, -bound), bound).astype(kind)


def setup_inputs(seed: int = 0) -> dict:
    streams_of = jax.random.split(jax.random.key(seed), 10)
    img_hidden = noise(streams_of[0], (BATCH, K_IMG), 0.03125, 0.25, ((0, 8), (1, 4)))
    img_down = noise(streams_of[1], (K_IMG, D), K_IMG ** -0.5, 0.09375, ((0, 4),))
    img_pooled = noise(streams_of[2], (BATCH, D), 0.03125, 0.25, ((0, 32),))
    txt_hidden = noise(streams_of[3], (BATCH, K_TXT), 0.03125, 0.25, ((0, 8), (1, 4)))
    txt_proj = noise(streams_of[4], (K_TXT, D), K_TXT ** -0.5, 0.1875, ((0, 4),))
    log_temp = jnp.clip(jax.random.uniform(streams_of[5], (1,), jnp.float32, 1.0, 2.0), 1.0, 2.0)
    bias = jnp.clip(jax.random.uniform(streams_of[6], (1,), jnp.float32, -4.0, -1.0), -4.0, -1.0)
    match = plant(jax.random.randint(streams_of[7], (BATCH,), 0, BATCH), jax.random.fold_in(streams_of[7], 1), 0, BATCH - 1).astype(jnp.int32)
    window_index = jax.random.randint(streams_of[8], (1,), 0, WINDOWS).astype(jnp.int32)
    return {"img_hidden": img_hidden, "img_down": img_down, "img_pooled": img_pooled, "txt_hidden": txt_hidden, "txt_proj": txt_proj, "log_temp": log_temp, "bias": bias, "match": match, "window_index": window_index}


def unit_rows(emb):
    length = jnp.sqrt(lax.optimization_barrier(jnp.sum(emb * emb, axis=1, keepdims=True)) + 1e-06)
    return (emb / length, length)

def reference(img_hidden, img_down, img_pooled, txt_hidden, txt_proj, log_temp, bias, match, window_index):
    img_emb = jnp.dot(img_hidden, img_down, preferred_element_type=jnp.float32) + img_pooled.astype(jnp.float32)
    txt_emb = jnp.dot(txt_hidden, txt_proj, preferred_element_type=jnp.float32)
    img_unit, img_len = unit_rows(img_emb)
    txt_unit, txt_len = unit_rows(txt_emb)
    blocks = N_DP * N_TENSOR
    image_low = img_unit.astype(jnp.bfloat16).astype(jnp.float32).reshape(blocks, ROWS, D)
    text_low = txt_unit.astype(jnp.bfloat16).astype(jnp.float32).reshape(blocks, ROWS, D)
    scale = jnp.exp(log_temp[0])
    shift_value = bias[0]
    base = window_index[0] * STEPS
    match_blocks = match.reshape(blocks, ROWS)
    owners_base = jnp.arange(blocks, dtype=jnp.int32)
    row_offsets = jnp.arange(ROWS, dtype=jnp.int32)
    image_dunit = jnp.zeros((blocks, ROWS, D), jnp.float32)
    text_dunit = jnp.zeros((blocks, ROWS, D), jnp.float32)
    row_loss = jnp.zeros((blocks, ROWS), jnp.float32)
    for offset_step in range(STEPS):
        offset = (base + offset_step).astype(jnp.int32)
        texts = jnp.roll(text_low, offset, axis=0)
        owners = (owners_base - offset) % blocks
        text_index = owners[:, None] * ROWS + row_offsets[None, :]
        positive = match_blocks[:, :, None] == text_index[:, None, :]
        cosine = jnp.einsum('prd,pqd->prq', image_low, texts)
        logit = scale * cosine + shift_value
        row_loss = row_loss + lax.optimization_barrier(jnp.sum(jnp.where(positive, jax.nn.softplus(-logit), jax.nn.softplus(logit)), axis=2))
        coef = ((jax.nn.sigmoid(logit) - positive.astype(jnp.float32)) * scale).astype(jnp.bfloat16).astype(jnp.float32)
        image_dunit = image_dunit + jnp.einsum('prq,pqd->prd', coef, texts)
        text_dunit = text_dunit + jnp.roll(jnp.einsum('prq,prd->pqd', coef, image_low), -offset, axis=0)
    image_dunit = image_dunit.reshape(BATCH, D)
    text_dunit = text_dunit.reshape(BATCH, D)
    img_grad = (image_dunit - img_unit * lax.optimization_barrier(jnp.sum(img_unit * image_dunit, axis=1, keepdims=True))) / img_len
    txt_grad = (text_dunit - txt_unit * lax.optimization_barrier(jnp.sum(txt_unit * text_dunit, axis=1, keepdims=True))) / txt_len
    return (img_grad, txt_grad, row_loss.reshape(BATCH))
```

```python
import jax
import jax.numpy as jnp
from jax import lax
from jax.sharding import PartitionSpec as P

STEPS = 16


def shifted(shard, axis, by):
    devices = lax.axis_size(axis)
    return lax.ppermute(shard, axis, [(i, (i + by) % devices) for i in range(devices)])


def unit_rows(emb):
    length = jnp.sqrt(jnp.sum(emb * emb, axis=1, keepdims=True) + 1e-06)
    return (emb / length, length)


def pair_tile(image_low, text_block, owner, match, scale, shift_value):
    cosine = lax.dot_general(
        image_low, text_block, (((1,), (1,)), ((), ())), preferred_element_type=jnp.float32
    )
    text_index = owner * text_block.shape[0] + lax.iota(jnp.int32, text_block.shape[0])
    positive = match[:, None] == text_index[None, :]
    logit = scale * cosine + shift_value
    pair_loss = jnp.sum(
        jnp.where(positive, jax.nn.softplus(-logit), jax.nn.softplus(logit)), axis=1
    )
    coef = ((jax.nn.sigmoid(logit) - positive.astype(jnp.float32)) * scale).astype(jnp.bfloat16)
    image_part = jnp.dot(coef, text_block, preferred_element_type=jnp.float32)
    text_part = lax.dot_general(
        coef, image_low, (((0,), (0,)), ((), ())), preferred_element_type=jnp.float32
    )
    return (pair_loss, image_part, text_part)


def offset_blocks(blocks, window):
    windows = lax.axis_size(("dp", "tensor")) // STEPS
    for level in range((windows - 1).bit_length()):
        moved = shifted(blocks, ("dp", "tensor"), STEPS << level)
        blocks = jnp.where(window >> level & 1 == 1, moved, blocks)
    return blocks


def return_home(text_sum, fixed_steps, window):
    text_sum = shifted(text_sum, ("dp", "tensor"), -fixed_steps)
    windows = lax.axis_size(("dp", "tensor")) // STEPS
    for level in range((windows - 1).bit_length()):
        moved = shifted(text_sum, ("dp", "tensor"), -(STEPS << level))
        text_sum = jnp.where(window >> level & 1 == 1, moved, text_sum)
    return text_sum


def ring_body(
    img_hidden, img_down, img_pooled, txt_hidden, txt_proj, log_temp, bias, match, window_index
):
    width = img_pooled.shape[1]
    summed = lax.psum_scatter(
        jnp.concatenate(
            [
                jnp.dot(img_hidden, img_down, preferred_element_type=jnp.float32),
                jnp.dot(txt_hidden, txt_proj, preferred_element_type=jnp.float32),
            ],
            axis=1,
        ),
        "tensor",
        scatter_dimension=0,
        tiled=True,
    )
    img_emb = summed[:, :width] + img_pooled.astype(jnp.float32)
    txt_emb = summed[:, width:]
    img_unit, img_len = unit_rows(img_emb)
    txt_unit, txt_len = unit_rows(txt_emb)
    image_low = img_unit.astype(jnp.bfloat16)
    text_low = txt_unit.astype(jnp.bfloat16)
    scale = jnp.exp(log_temp[0])
    shift_value = bias[0]
    window = window_index[0]
    start_step = window * STEPS
    position = lax.axis_index(("dp", "tensor"))
    devices = lax.axis_size(("dp", "tensor"))
    half_steps = STEPS // 2
    late_copy = shifted(text_low, ("dp", "tensor"), STEPS - 1)
    stacked = offset_blocks(jnp.stack([text_low, late_copy]), window)
    early_block = stacked[0]
    late_block = stacked[1]
    early_owner = (position - start_step) % devices
    late_owner = (position - start_step - (STEPS - 1)) % devices
    early_loss, early_image, early_sum = pair_tile(
        image_low, early_block, early_owner, match, scale, shift_value
    )
    late_loss, late_image, late_sum = pair_tile(
        image_low, late_block, late_owner, match, scale, shift_value
    )

    def two_turn(turn, carry):
        early_now, late_now, early_acc, late_acc, image_now, loss_now = carry
        early_now = shifted(early_now, ("dp", "tensor"), 1)
        late_now = shifted(late_now, ("dp", "tensor"), -1)
        early_acc = shifted(early_acc, ("dp", "tensor"), 1)
        late_acc = shifted(late_acc, ("dp", "tensor"), -1)
        owner_early = (position - start_step - turn) % devices
        owner_late = (position - start_step - (STEPS - 1) + turn) % devices
        loss_one, image_one, text_one = pair_tile(
            image_low, early_now, owner_early, match, scale, shift_value
        )
        loss_two, image_two, text_two = pair_tile(
            image_low, late_now, owner_late, match, scale, shift_value
        )
        return (
            early_now,
            late_now,
            early_acc + text_one,
            late_acc + text_two,
            image_now + image_one + image_two,
            loss_now + loss_one + loss_two,
        )

    carried = lax.fori_loop(
        1,
        half_steps,
        two_turn,
        (
            early_block,
            late_block,
            early_sum,
            late_sum,
            early_image + late_image,
            early_loss + late_loss,
        ),
    )
    early_sum = carried[2]
    late_sum = carried[3]
    image_dunit = carried[4]
    row_loss = carried[5]
    late_moved = shifted(late_sum, ("dp", "tensor"), -1)
    text_dunit = return_home(early_sum + late_moved, half_steps - 1, window)
    img_grad = (
        image_dunit - img_unit * jnp.sum(img_unit * image_dunit, axis=1, keepdims=True)
    ) / img_len
    txt_grad = (
        text_dunit - txt_unit * jnp.sum(txt_unit * text_dunit, axis=1, keepdims=True)
    ) / txt_len
    return (img_grad, txt_grad, row_loss)


def scatter_sum(partial, axis):
    parts = lax.axis_size(axis)
    rows = partial.shape[0] // parts
    pieces = partial.astype(jnp.bfloat16).reshape(parts, rows, partial.shape[1])
    got = lax.all_to_all(pieces, axis, 0, 0).astype(jnp.float32)
    return jnp.sum(got, axis=0)


def stable_terms(logit, positive):
    signed = jnp.where(positive, -logit, logit)
    small = jnp.exp(-jnp.abs(signed))
    loss = jnp.maximum(signed, 0.0) + jnp.log1p(small)
    chance = jnp.where(signed >= 0.0, 1.0, small) / (1.0 + small)
    return loss, jnp.where(positive, -chance, chance)


def tangent(dunit, unit, length):
    return (dunit - unit * jnp.sum(unit * dunit, axis=1, keepdims=True)) / length


def gather_body(
    img_hidden, img_down, img_pooled, txt_hidden, txt_proj, log_temp, bias, match, window_index
):
    both = ("dp", "tensor")
    width = img_pooled.shape[1]
    rows = img_pooled.shape[0]
    devices = lax.axis_size(both)
    position = lax.axis_index(both)
    txt_emb = scatter_sum(jnp.dot(txt_hidden, txt_proj, preferred_element_type=jnp.float32), "tensor")
    img_emb = scatter_sum(
        jnp.dot(img_hidden, img_down, preferred_element_type=jnp.float32), "tensor"
    ) + img_pooled.astype(jnp.float32)
    img_unit, img_len = unit_rows(img_emb)
    txt_unit, txt_len = unit_rows(txt_emb)
    image_low = img_unit.astype(jnp.bfloat16)
    text_low = txt_unit.astype(jnp.bfloat16)
    texts = lax.all_gather(text_low, both, axis=0, tiled=True)
    images = lax.all_gather(image_low, both, axis=0, tiled=True)
    matches = lax.all_gather(match, both, axis=0, tiled=True)
    scale = jnp.exp(log_temp[0])
    shift_value = bias[0]
    window = window_index[0]
    every = lax.iota(jnp.int32, devices * rows)
    own = position * rows + lax.iota(jnp.int32, rows)
    nt = (((1,), (1,)), ((), ()))

    logit = scale * lax.dot_general(image_low, texts, nt, preferred_element_type=jnp.float32) + shift_value
    offset = (position - every // rows) % devices
    inside = (offset // STEPS == window)[None, :]
    loss, slope = stable_terms(logit, match[:, None] == every[None, :])
    row_loss = jnp.sum(jnp.where(inside, loss, 0.0), axis=1)
    coef = jnp.where(inside, slope * scale, 0.0).astype(jnp.bfloat16)
    image_dunit = jnp.dot(coef, texts, preferred_element_type=jnp.float32)

    logit = scale * lax.dot_general(text_low, images, nt, preferred_element_type=jnp.float32) + shift_value
    offset = (every // rows - position) % devices
    inside = (offset // STEPS == window)[None, :]
    _, slope = stable_terms(logit, matches[None, :] == own[:, None])
    coef = jnp.where(inside, slope * scale, 0.0).astype(jnp.bfloat16)
    text_dunit = jnp.dot(coef, images, preferred_element_type=jnp.float32)
    return (
        tangent(image_dunit, img_unit, img_len),
        tangent(text_dunit, txt_unit, txt_len),
        row_loss,
    )


def solution(mesh):
    in_specs = (
        P("dp", "tensor"),
        P("tensor", None),
        P(("dp", "tensor"), None),
        P("dp", "tensor"),
        P("tensor", None),
        P(),
        P(),
        P(("dp", "tensor")),
        P(),
    )
    out_specs = (P(("dp", "tensor"), None), P(("dp", "tensor"), None), P(("dp", "tensor")))
    whole = mesh.shape["dp"] * mesh.shape["tensor"]
    body = gather_body if whole <= 2 * STEPS else ring_body
    return jax.shard_map(body, mesh=mesh, in_specs=in_specs, out_specs=out_specs, check_vma=False)
```

```python
import jax
import jax.numpy as jnp
from jax import lax
from jax.experimental import pallas as pl
from jax.experimental.pallas import tpu as pltpu
from jax.sharding import PartitionSpec as P

STEPS = 16


def shifted(shard, axis, by):
    devices = lax.axis_size(axis)
    return lax.ppermute(shard, axis, [(i, (i + by) % devices) for i in range(devices)])


def unit_rows(emb):
    length = jnp.sqrt(jnp.sum(emb * emb, axis=1, keepdims=True) + 1e-06)
    return (emb / length, length)


def pair_tile(image_low, text_block, owner, match, scale, shift_value):
    cosine = lax.dot_general(
        image_low, text_block, (((1,), (1,)), ((), ())), preferred_element_type=jnp.float32
    )
    text_index = owner * text_block.shape[0] + lax.iota(jnp.int32, text_block.shape[0])
    positive = match[:, None] == text_index[None, :]
    logit = scale * cosine + shift_value
    pair_loss = jnp.sum(
        jnp.where(positive, jax.nn.softplus(-logit), jax.nn.softplus(logit)), axis=1
    )
    coef = ((jax.nn.sigmoid(logit) - positive.astype(jnp.float32)) * scale).astype(jnp.bfloat16)
    image_part = jnp.dot(coef, text_block, preferred_element_type=jnp.float32)
    text_part = lax.dot_general(
        coef, image_low, (((0,), (0,)), ((), ())), preferred_element_type=jnp.float32
    )
    return (pair_loss, image_part, text_part)


def offset_blocks(blocks, window):
    windows = lax.axis_size(("dp", "tensor")) // STEPS
    for level in range((windows - 1).bit_length()):
        moved = shifted(blocks, ("dp", "tensor"), STEPS << level)
        blocks = jnp.where(window >> level & 1 == 1, moved, blocks)
    return blocks


def return_home(text_sum, fixed_steps, window):
    text_sum = shifted(text_sum, ("dp", "tensor"), -fixed_steps)
    windows = lax.axis_size(("dp", "tensor")) // STEPS
    for level in range((windows - 1).bit_length()):
        moved = shifted(text_sum, ("dp", "tensor"), -(STEPS << level))
        text_sum = jnp.where(window >> level & 1 == 1, moved, text_sum)
    return text_sum


def ring_body(
    img_hidden, img_down, img_pooled, txt_hidden, txt_proj, log_temp, bias, match, window_index
):
    width = img_pooled.shape[1]
    summed = lax.psum_scatter(
        jnp.concatenate(
            [
                jnp.dot(img_hidden, img_down, preferred_element_type=jnp.float32),
                jnp.dot(txt_hidden, txt_proj, preferred_element_type=jnp.float32),
            ],
            axis=1,
        ),
        "tensor",
        scatter_dimension=0,
        tiled=True,
    )
    img_emb = summed[:, :width] + img_pooled.astype(jnp.float32)
    txt_emb = summed[:, width:]
    img_unit, img_len = unit_rows(img_emb)
    txt_unit, txt_len = unit_rows(txt_emb)
    image_low = img_unit.astype(jnp.bfloat16)
    text_low = txt_unit.astype(jnp.bfloat16)
    scale = jnp.exp(log_temp[0])
    shift_value = bias[0]
    window = window_index[0]
    start_step = window * STEPS
    position = lax.axis_index(("dp", "tensor"))
    devices = lax.axis_size(("dp", "tensor"))
    half_steps = STEPS // 2
    late_copy = shifted(text_low, ("dp", "tensor"), STEPS - 1)
    stacked = offset_blocks(jnp.stack([text_low, late_copy]), window)
    early_block = stacked[0]
    late_block = stacked[1]
    early_owner = (position - start_step) % devices
    late_owner = (position - start_step - (STEPS - 1)) % devices
    early_loss, early_image, early_sum = pair_tile(
        image_low, early_block, early_owner, match, scale, shift_value
    )
    late_loss, late_image, late_sum = pair_tile(
        image_low, late_block, late_owner, match, scale, shift_value
    )

    def two_turn(turn, carry):
        early_now, late_now, early_acc, late_acc, image_now, loss_now = carry
        early_now = shifted(early_now, ("dp", "tensor"), 1)
        late_now = shifted(late_now, ("dp", "tensor"), -1)
        early_acc = shifted(early_acc, ("dp", "tensor"), 1)
        late_acc = shifted(late_acc, ("dp", "tensor"), -1)
        owner_early = (position - start_step - turn) % devices
        owner_late = (position - start_step - (STEPS - 1) + turn) % devices
        loss_one, image_one, text_one = pair_tile(
            image_low, early_now, owner_early, match, scale, shift_value
        )
        loss_two, image_two, text_two = pair_tile(
            image_low, late_now, owner_late, match, scale, shift_value
        )
        return (
            early_now,
            late_now,
            early_acc + text_one,
            late_acc + text_two,
            image_now + image_one + image_two,
            loss_now + loss_one + loss_two,
        )

    carried = lax.fori_loop(
        1,
        half_steps,
        two_turn,
        (
            early_block,
            late_block,
            early_sum,
            late_sum,
            early_image + late_image,
            early_loss + late_loss,
        ),
    )
    early_sum = carried[2]
    late_sum = carried[3]
    image_dunit = carried[4]
    row_loss = carried[5]
    late_moved = shifted(late_sum, ("dp", "tensor"), -1)
    text_dunit = return_home(early_sum + late_moved, half_steps - 1, window)
    img_grad = (
        image_dunit - img_unit * jnp.sum(img_unit * image_dunit, axis=1, keepdims=True)
    ) / img_len
    txt_grad = (
        text_dunit - txt_unit * jnp.sum(txt_unit * text_dunit, axis=1, keepdims=True)
    ) / txt_len
    return (img_grad, txt_grad, row_loss)


def scatter_sum(partial, axis):
    parts = lax.axis_size(axis)
    rows = partial.shape[0] // parts
    pieces = partial.astype(jnp.bfloat16).reshape(parts, rows, partial.shape[1])
    got = lax.all_to_all(pieces, axis, 0, 0).astype(jnp.float32)
    return jnp.sum(got, axis=0)


def stable_terms(logit, positive):
    signed = jnp.where(positive, -logit, logit)
    small = jnp.exp(-jnp.abs(signed))
    loss = jnp.maximum(signed, 0.0) + jnp.log1p(small)
    chance = jnp.where(signed >= 0.0, 1.0, small) / (1.0 + small)
    return loss, jnp.where(positive, -chance, chance)


def tangent(dunit, unit, length):
    return (dunit - unit * jnp.sum(unit * dunit, axis=1, keepdims=True)) / length


def exchange(pay, out, twin, col, z_send, z_recv, p_send, f_send, out_recv, twin_recv, local_sem):
    dp = lax.axis_index("dp")
    z = lax.axis_index("tensor")
    depth = lax.axis_size("tensor")
    devices = lax.axis_size("dp") * depth
    half = devices // 2
    y, x, c = dp // 4, (dp // 2) % 2, dp % 2

    def group(y, x, c):
        return y * 4 + x * 2 + c

    def slot(kind, source, target):
        ahead = (1 - 2 * kind) * (target - source)
        return kind * (half - 1) + lax.rem(ahead + devices, devices) - 1

    peers = [
        group(y, x, 1 - c),
        group(y, 1 - x, c),
        group(1 - y, 1 - x, c),
        group(1 - y, x, 1 - c),
        group(1 - y, x, c),
    ]
    barrier = pltpu.get_barrier_semaphore()
    for peer in peers:
        pl.semaphore_signal(barrier, inc=1, device_id=(peer, z), device_id_type=pl.DeviceIdType.MESH)
    has_up = z < depth - 1
    has_down = z > 0

    @pl.when(has_up)
    def _():
        pl.semaphore_signal(barrier, inc=1, device_id=(dp, z + 1), device_id_type=pl.DeviceIdType.MESH)

    @pl.when(has_down)
    def _():
        pl.semaphore_signal(barrier, inc=1, device_id=(dp, z - 1), device_id_type=pl.DeviceIdType.MESH)

    inner = jnp.logical_and(has_up, has_down)

    @pl.when(inner)
    def _():
        pl.semaphore_wait(barrier, len(peers) + 2)

    @pl.when(jnp.logical_not(inner))
    def _():
        pl.semaphore_wait(barrier, len(peers) + 1)

    started = []

    def start(condition, make):
        @pl.when(condition)
        def _():
            make().start()

        started.append((condition, make))

    def remote(source, target, send, recv, peer, level):
        return lambda: pltpu.make_async_remote_copy(
            src_ref=source(),
            dst_ref=target(),
            send_sem=send(),
            recv_sem=recv(),
            device_id=(peer, level),
            device_id_type=pl.DeviceIdType.MESH,
        )

    def arrived(condition, index):
        @pl.when(condition)
        def _():
            pltpu.make_async_remote_copy(
                src_ref=out.at[index],
                dst_ref=out.at[index],
                send_sem=f_send.at[0, 0],
                recv_sem=out_recv.at[index],
                device_id=(peers[0], z),
                device_id_type=pl.DeviceIdType.MESH,
            ).wait_recv()

    def along(tag, level, kind, way, condition):
        held = (lambda: pay.at[kind]) if tag == 0 else (lambda: col.at[level, kind])
        start(
            condition,
            remote(
                held,
                lambda: col.at[level, kind],
                lambda: z_send.at[tag, kind, way],
                lambda: z_recv.at[level, kind],
                dp,
                z + 1 - 2 * way,
            ),
        )

    def spread(tag, level, condition):
        source = dp * depth + level

        def send(job, kind, peer, when):
            index = slot(kind, source, peer * depth + z)
            held = (lambda: pay.at[kind]) if tag == 0 else (lambda: col.at[level, kind])
            start(
                when,
                remote(
                    held,
                    lambda: out.at[index],
                    lambda: p_send.at[tag, job],
                    lambda: out_recv.at[index],
                    peer,
                    z,
                ),
            )

        send(0, 1 - c, peers[3], condition)
        send(1, 1 - x, peers[2], condition)
        send(2, x, peers[1], condition)
        send(3, c, peers[0], condition)
        if tag == 0:
            for kind in (0, 1):
                start(
                    condition,
                    remote(
                        lambda kind=kind: pay.at[kind],
                        lambda kind=kind: twin.at[kind],
                        lambda kind=kind: p_send.at[0, 4 + kind],
                        lambda kind=kind: twin_recv.at[kind],
                        peers[4],
                        z,
                    ),
                )
        else:
            below = tag % 2
            send(4, c, peers[4], jnp.logical_and(condition, c == below))

    def keep(tag, level, condition):
        kind = 1 - tag % 2
        index = slot(kind, dp * depth + level, dp * depth + z)

        @pl.when(condition)
        def _():
            pltpu.make_async_copy(col.at[level, kind], out.at[index], local_sem.at[tag]).start()

    def kept(tag, level, condition):
        kind = 1 - tag % 2
        index = slot(kind, dp * depth + level, dp * depth + z)

        @pl.when(condition)
        def _():
            pltpu.make_async_copy(col.at[level, kind], out.at[index], local_sem.at[tag]).wait()

    def relay(tag, level, condition):
        me = dp * depth + z
        other = peers[0] * depth + z

        def hand(job, kind, origin, when, onward):
            source = origin * depth + level
            arrived(when, slot(kind, source, me))
            if onward is not None:
                index = slot(kind, source, me)
                landing = slot(kind, source, other)
                start(
                    onward,
                    remote(
                        lambda: out.at[index],
                        lambda: out.at[landing],
                        lambda: f_send.at[tag, job],
                        lambda: out_recv.at[landing],
                        peers[0],
                        z,
                    ),
                )

        hand(0, 1 - x, peers[1], condition, condition)
        hand(1, x, peers[2], condition, condition)
        onward = None if tag == 0 else jnp.logical_and(condition, c == tag % 2)
        hand(2, c, peers[3], condition, onward)

    def finish(tag, level, condition):
        me = dp * depth + z
        arrived(condition, slot(1 - c, peers[0] * depth + level, me))
        arrived(condition, slot(1 - x, group(y, 1 - x, 1 - c) * depth + level, me))
        arrived(condition, slot(x, group(1 - y, 1 - x, 1 - c) * depth + level, me))
        if tag:
            arrived(condition, slot(tag % 2, peers[4] * depth + level, me))

    always = z >= 0
    for kind in (0, 1):
        along(0, z, kind, 0, has_up)
        along(0, z, kind, 1, has_down)
    spread(0, z, always)
    turns = [(0, z, always)]
    for hop in range(1, depth):
        here = []
        for way in (0, 1):
            level = z - hop if way == 0 else z + hop
            condition = level >= 0 if way == 0 else level < depth
            tag = 2 * hop - 1 if way == 0 else 2 * hop
            for kind in (0, 1):

                @pl.when(condition)
                def _():
                    pltpu.make_async_remote_copy(
                        src_ref=col.at[level, kind],
                        dst_ref=col.at[level, kind],
                        send_sem=f_send.at[0, 0],
                        recv_sem=z_recv.at[level, kind],
                        device_id=(peers[0], z),
                        device_id_type=pl.DeviceIdType.MESH,
                    ).wait_recv()

                if hop < depth - 1:
                    more = has_up if way == 0 else has_down
                    along(tag, level, kind, way, jnp.logical_and(condition, more))
            spread(tag, level, condition)
            keep(tag, level, condition)
            here.append((tag, level, condition))
        for turn in turns[-2 if hop > 1 else -1 :]:
            relay(*turn)
        turns += here
    for turn in turns[-2:]:
        relay(*turn)
    for turn in turns:
        finish(*turn)
        if turn[0]:
            kept(*turn)
    for kind in (0, 1):
        pltpu.make_async_remote_copy(
            src_ref=twin.at[kind],
            dst_ref=twin.at[kind],
            send_sem=f_send.at[0, 0],
            recv_sem=twin_recv.at[kind],
            device_id=(peers[4], z),
            device_id_type=pl.DeviceIdType.MESH,
        ).wait_recv()
    for condition, make in started:

        @pl.when(condition)
        def _():
            make().wait_send()


def swap_blocks(pay):
    devices = lax.axis_size(("dp", "tensor"))
    depth = lax.axis_size("tensor")
    slots = devices - 2
    tags = 2 * depth - 1
    block = pay.shape[1:]
    dma = pltpu.SemaphoreType.DMA
    return pl.pallas_call(
        exchange,
        out_shape=(
            jax.ShapeDtypeStruct((slots,) + block, pay.dtype),
            jax.ShapeDtypeStruct((2,) + block, pay.dtype),
        ),
        in_specs=[pl.BlockSpec(memory_space=pltpu.VMEM)],
        out_specs=(pl.BlockSpec(memory_space=pl.ANY), pl.BlockSpec(memory_space=pl.ANY)),
        scratch_shapes=[
            pltpu.VMEM((depth, 2) + block, pay.dtype),
            dma((tags, 2, 2)),
            dma((depth, 2)),
            dma((tags, 6)),
            dma((tags, 3)),
            dma((slots,)),
            dma((2,)),
            dma((tags,)),
        ],
        compiler_params=pltpu.CompilerParams(collective_id=1, has_side_effects=True),
    )(pay)


def gather_body(
    img_hidden, img_down, img_pooled, txt_hidden, txt_proj, log_temp, bias, match, window_index
):
    both = ("dp", "tensor")
    width = img_pooled.shape[1]
    rows = img_pooled.shape[0]
    devices = lax.axis_size(both)
    position = lax.axis_index(both)
    txt_emb = scatter_sum(jnp.dot(txt_hidden, txt_proj, preferred_element_type=jnp.float32), "tensor")
    img_emb = scatter_sum(
        jnp.dot(img_hidden, img_down, preferred_element_type=jnp.float32), "tensor"
    ) + img_pooled.astype(jnp.float32)
    img_unit, img_len = unit_rows(img_emb)
    txt_unit, txt_len = unit_rows(txt_emb)
    image_low = img_unit.astype(jnp.bfloat16)
    text_low = txt_unit.astype(jnp.bfloat16)
    matches = lax.all_gather(match, both, axis=0, tiled=True).reshape(devices, rows)
    scale = jnp.exp(log_temp[0])
    shift_value = bias[0]
    first = window_index[0] == 0
    pay = jnp.where(first, jnp.stack([text_low, image_low]), jnp.stack([image_low, text_low]))
    slots, twin = swap_blocks(pay)
    count = devices // 2 - 1
    start = jnp.where(first, pay, twin)
    away = jnp.where(first, 0, devices // 2)
    own = position * rows + lax.iota(jnp.int32, rows)
    steps = 1 + lax.iota(jnp.int32, count)

    def side(kind, left, sign, texts_here):
        far = slots[kind * count : (kind + 1) * count].reshape(count * rows, -1)
        near = start[kind]
        owners = jnp.concatenate([(position + away)[None], position - sign * steps]) % devices
        columns = (owners[:, None] * rows + lax.iota(jnp.int32, rows)[None, :]).reshape(-1)
        wanted = jnp.where(texts_here, match, own)
        offered = jnp.where(texts_here, columns, matches[owners].reshape(-1))
        nt = (((1,), (1,)), ((), ()))

        def part(block, offered):
            cosine = lax.dot_general(left, block, nt, preferred_element_type=jnp.float32)
            logit = scale * cosine + shift_value
            loss, slope = stable_terms(logit, wanted[:, None] == offered[None, :])
            coef = (slope * scale).astype(jnp.bfloat16)
            return jnp.sum(loss, axis=1), jnp.dot(coef, block, preferred_element_type=jnp.float32)

        near_loss, near_sum = part(near, offered[:rows])
        far_loss, far_sum = part(far, offered[rows:])
        return near_loss + far_loss, near_sum + far_sum

    loss_a, sum_a = side(0, pay[1], 1, first)
    loss_b, sum_b = side(1, pay[0], -1, jnp.logical_not(first))
    return (
        tangent(jnp.where(first, sum_a, sum_b), img_unit, img_len),
        tangent(jnp.where(first, sum_b, sum_a), txt_unit, txt_len),
        jnp.where(first, loss_a, loss_b),
    )


def solution(mesh):
    in_specs = (
        P("dp", "tensor"),
        P("tensor", None),
        P(("dp", "tensor"), None),
        P("dp", "tensor"),
        P("tensor", None),
        P(),
        P(),
        P(("dp", "tensor")),
        P(),
    )
    out_specs = (P(("dp", "tensor"), None), P(("dp", "tensor"), None), P(("dp", "tensor")))
    whole = mesh.shape["dp"] * mesh.shape["tensor"]
    body = gather_body if whole == 2 * STEPS and mesh.shape["dp"] == 8 else ring_body
    return jax.shard_map(body, mesh=mesh, in_specs=in_specs, out_specs=out_specs, check_vma=False)
```
